32 devices in a mesh: dp: 4 (over y, x), vocab: 8 (over z, core).
Axes of the slice: x: 2, y: 2, z: 4, core: 2. Of those that a mesh axis runs over, the one named last changes fastest.
Arguments:
- logits: bfloat16 [32, 8, 152064], P('dp', None, 'vocab'), may hold values from -40 to 250
- draft_probs: bfloat16 [32, 8, 152064], P('dp', None, 'vocab'), may hold values from 5.9185606e-07 to 1, as said below
- draft_tokens: int32 [32, 8], P('dp'), may hold values from 0 to 152063
- draft_lengths: int32 [32], P('dp'), may hold values from 1 to 8
- owner_group: int32 [32], P('dp'), may hold values from 0 to 3, as said below
Outputs:
- correction: bfloat16 [64, 152064], P('dp', 'vocab')
- accept_ratio: float32 [64, 8], P('dp')
- expected_accepted: float32 [64], P('dp')
The draws below stay inside these ranges and needn't reach their ends.
Inputs may be any that keep to these rules, and one draw needn't show every extreme that they name: Each row of draft_probs is a distribution over the whole vocabulary whose entries are all positive. `owner_group`: no group hands more than 4 sequences to one group; some group receives exactly 4 sequences from every group.
All inputs are finite; a program needn't handle non-finite values.
Results may differ from the reference program's by a relative error of at most 0.001.
Values may be sent and summed in bfloat16 or wider, within the bound.
A program may use at most 64 MiB of HBM per device.

```python
import math
import jax
import jax.numpy as jnp
from jax import lax

VOCAB = 152064
DRAFT_MAX = 8
SEQ_DEV = 8
CAP = 4
SEQS = 32
SLOTS = 64
N_DP = 4


def logit_field(key):
    root_key = jax.random.fold_in(key, 11)
    key_base = jax.random.fold_in(root_key, 1)
    key_rows = jax.random.fold_in(root_key, 2)
    key_cols = jax.random.fold_in(root_key, 3)
    shape = (SEQS, DRAFT_MAX, VOCAB)
    row_scale = jnp.exp(jax.random.uniform(key_rows, (SEQS, DRAFT_MAX, 1), jnp.float32, math.log(1.5), math.log(4.0)))
    col_scale = jnp.exp(jax.random.uniform(key_cols, (1, 1, VOCAB), jnp.float32, 0.0, math.log(3.2)))
    base = jax.random.normal(key_base, shape, jnp.float32)
    scores = jnp.clip(base * row_scale * col_scale, -40.0, 40.0)
    return scores


def draw_logits(key, part):
    return logit_field(key).astype(jnp.bfloat16)


def draw_draft_probs(key, part):
    scores = logit_field(key)
    noise = 1.5 * jax.random.normal(jax.random.fold_in(key, 23), scores.shape, jnp.float32)
    proposal = jax.nn.softmax(0.7 * scores + noise, axis=2)
    return (0.9 * proposal + 0.1 / VOCAB).astype(jnp.bfloat16)


def draw_owner_group(key, part):
    groups = SEQS // SEQ_DEV
    root_key = jax.random.fold_in(key, 31)
    favoured = jax.random.randint(jax.random.fold_in(root_key, 1), (), 0, groups)
    slot_owner = jnp.arange(groups * CAP, dtype=jnp.int32) // CAP
    block_keys = jax.random.split(jax.random.fold_in(root_key, 2), groups)

    def one_block(block_key):
        key_order = jax.random.fold_in(block_key, 1)
        key_shuffle = jax.random.fold_in(block_key, 2)
        shuffle = jax.random.permutation(key_order, groups * CAP).astype(jnp.int32)
        priority = jnp.where(slot_owner == favoured, -1, shuffle)
        picked = jnp.argsort(priority, stable=True)[:SEQ_DEV]
        owners = slot_owner[picked]
        return owners[jax.random.permutation(key_shuffle, SEQ_DEV)]
    return jax.vmap(one_block)(block_keys).reshape(SEQS).astype(jnp.int32)


def touch_ends(values, key, least, top_value):
    spot = [jax.random.randint(jax.random.fold_in(key, axis), (), 0, length) for axis, length in enumerate(values.shape)]
    widest = values.shape.index(max(values.shape))
    beside = spot[:widest] + [(spot[widest] + 1) % values.shape[widest]] + spot[widest + 1:]
    return values.at[tuple(spot)].set(least).at[tuple(beside)].set(top_value)


def setup_inputs(seed: int = 0) -> dict:
    arg_keys = jax.random.split(jax.random.key(seed), 6)
    return {
        "logits": draw_logits(jax.random.fold_in(arg_keys[5], 71), 0),
        "draft_probs": draw_draft_probs(jax.random.fold_in(arg_keys[5], 71), 0),
        "draft_tokens": touch_ends(jax.random.randint(arg_keys[2], (SEQS, DRAFT_MAX), 0, VOCAB), jax.random.fold_in(arg_keys[2], 1), 0, VOCAB - 1).astype(jnp.int32),
        "draft_lengths": touch_ends(jax.random.randint(arg_keys[3], (SEQS,), 1, DRAFT_MAX + 1), jax.random.fold_in(arg_keys[3], 1), 1, DRAFT_MAX).astype(jnp.int32),
        "owner_group": draw_owner_group(jax.random.fold_in(arg_keys[5], 71), 0),
    }


mixing = 0.1


def verify_group(packed):
    logits, draft_probs, tokens, lengths = packed
    scores = logits.astype(jnp.float32)
    top = jnp.max(scores, axis=2)
    shifted = jnp.exp(scores - top[:, :, None])
    row_total = jnp.sum(shifted, axis=2)
    target = shifted / row_total[:, :, None]
    proposal = draft_probs.astype(jnp.float32)
    index = tokens[:, :, None].astype(jnp.int32)
    picked_target = jnp.take_along_axis(target, index, axis=2)[:, :, 0]
    picked_draft = jnp.take_along_axis(proposal, index, axis=2)[:, :, 0]
    position = lax.broadcasted_iota(jnp.int32, tokens.shape, 1)
    is_live = position < lengths[:, None]
    safe_draft = jnp.where(is_live, picked_draft, 1.0)
    accept = jnp.where(is_live, jnp.minimum(1.0, picked_target / safe_draft), 0.0)
    excess = jnp.maximum(target - proposal, 0.0)
    spread = jnp.sum(excess, axis=2)
    residual = (excess + mixing * target) / (spread + mixing)[:, :, None]
    survive = jnp.cumprod(accept, axis=1)
    before = jnp.concatenate([jnp.ones_like(survive[:, :1]), survive[:, :-1]], axis=1)
    weight = jnp.where(is_live, before * (1.0 - accept), 0.0)
    corrected = jnp.sum(weight[:, :, None] * residual, axis=1).astype(jnp.bfloat16)
    expected = jnp.sum(survive, axis=1)
    return corrected, accept, expected


def reference(logits, draft_probs, draft_tokens, draft_lengths, owner_group):
    grouped = (logits.reshape(N_DP, SEQ_DEV, DRAFT_MAX, VOCAB),
               draft_probs.reshape(N_DP, SEQ_DEV, DRAFT_MAX, VOCAB),
               draft_tokens.reshape(N_DP, SEQ_DEV, DRAFT_MAX),
               draft_lengths.reshape(N_DP, SEQ_DEV))
    corrected, accept, expected = lax.map(verify_group, grouped)
    owners = owner_group.reshape(N_DP, SEQ_DEV).astype(jnp.int32)
    position = jnp.arange(SEQ_DEV, dtype=jnp.int32)
    earlier = position[None, :] < position[:, None]
    same = owners[:, :, None] == owners[:, None, :]
    slot_rank = jnp.sum(jnp.where(same & earlier[None], 1, 0), axis=2).astype(jnp.int32)
    source = jnp.arange(N_DP, dtype=jnp.int32)[:, None]
    landing = (owners * (N_DP * CAP) + source * CAP + slot_rank).reshape(SEQS).astype(jnp.int32)
    correction = jnp.zeros((SLOTS, VOCAB), corrected.dtype).at[landing].set(corrected.reshape(SEQS, VOCAB))
    accept_ratio = jnp.zeros((SLOTS, DRAFT_MAX), accept.dtype).at[landing].set(accept.reshape(SEQS, DRAFT_MAX))
    expected_accepted = jnp.zeros((SLOTS,), expected.dtype).at[landing].set(expected.reshape(SEQS))
    return correction, accept_ratio, expected_accepted
```

```python
import functools

import jax
import jax.numpy as jnp
from jax import lax
from jax.experimental import pallas as pl
from jax.experimental.pallas import tpu as pltpu
from jax.sharding import PartitionSpec as P

mixing = 0.1
LANES = 128
SLAB = 8
PIECE = 2
BATCHES = 1
TERMS = 3
PAIR = 2
FIRST = 6
GROWTH = 3
MOST = 40
LOW = -1e30
MESH = pl.DeviceIdType.MESH
scope = jax.named_scope


def slabs(full, size):
    return [(a, min(size, full - a)) for a in range(0, full, size)]


def plan(tiles):
    bounds, size = [0], FIRST
    while bounds[-1] < tiles:
        bounds.append(min(tiles, bounds[-1] + size))
        size = min(size * GROWTH, MOST)
    return bounds


def xor(value, mask):
    bit = 1
    while bit <= mask:
        if mask & bit:
            value = value + bit - 2 * bit * lax.rem(value // bit, 2)
        bit *= 2
    return value


def partners(me, count):
    if count & (count - 1):
        return [lax.rem(me + k, count) for k in range(1, count)]
    return [xor(me, k) for k in range(count - 1, 0, -1)]


def tree(op, values):
    values = list(values)
    while len(values) > 1:
        values = [op(*values[i:i + 2]) if i + 1 < len(values) else values[i] for i in range(0, len(values), 2)]
    return values[0]


def kernel(
    dims,
    tok_hbm, lens_hbm, own_hbm, x_hbm, d_hbm,
    block, accept_out, expected_out,
    tok, lens, own, x, d, e, send, landed, comm, small, small_in,
    scalar_sem, x_sem, d_sem, comm_ssem, comm_rsem, out_ssem, out_rsem, sm_ssem, sm_rsem,
):
    groups, vocab, capacity = dims
    seqs, depth, width = x_hbm.shape
    full = width // LANES
    tail = width - full * LANES
    tiles = e.shape[2] // LANES
    rows = seqs * depth
    slots = groups * capacity
    half = LANES // 2
    pick_slot, norm_slot = BATCHES, BATCHES + 1
    my_dp = lax.axis_index("dp")
    my_v = lax.axis_index("vocab")

    pairs = slabs(seqs, PAIR)
    x_loads, d_loads = [], []
    for i, (n, size) in enumerate(pairs):
        part = pl.ds(n, size)
        x_loads.append(pltpu.make_async_copy(x_hbm.at[part], x.at[part], x_sem.at[i]))
        d_loads.append(pltpu.make_async_copy(d_hbm.at[part], d.at[part], d_sem))
        x_loads[-1].start()
    scalars = []
    for i, (source, target) in enumerate(((tok_hbm, tok), (lens_hbm, lens), (own_hbm, own))):
        scalars.append(pltpu.make_async_copy(source, target, scalar_sem.at[i]))
        scalars[-1].start()

    barrier = pltpu.get_barrier_semaphore()
    v_peers = [lax.rem(my_v + k, vocab) for k in range(1, vocab)]
    g_peers = partners(my_dp, groups)
    for p in v_peers:
        pl.semaphore_signal(barrier, inc=1, device_id=(my_dp, p), device_id_type=MESH)
    for p in g_peers:
        pl.semaphore_signal(barrier, inc=1, device_id=(p, my_v), device_id_type=MESH)

    sub = lax.broadcasted_iota(jnp.int32, (depth, LANES), 0)
    lane = lax.broadcasted_iota(jnp.int32, (depth, LANES), 1)
    row_lane = lax.broadcasted_iota(jnp.int32, (1, LANES), 1)
    lane_j = lax.rem(row_lane, depth)
    lane_n = lax.rem(row_lane // depth, seqs)
    zero = jnp.zeros((depth, LANES), jnp.float32)
    spots = [(lax.rem(lane, depth) == sub) & (lax.rem(lane // depth, seqs) == n) for n in range(seqs)]

    def tail_tile(ref, n, fill):
        part = ref[n, :, pl.ds(full * LANES, tail)].astype(jnp.float32)
        return jnp.concatenate([part, jnp.full((depth, LANES - tail), fill, jnp.float32)], axis=1)

    def to_row(columns):
        spread = zero
        for n, column in columns.items():
            spread = jnp.where(spots[n], column, spread)
        return jnp.sum(spread, axis=0, keepdims=True)

    def to_column(row, n):
        placed = jnp.where(spots[n] & (lane < rows), row, 0.0)
        return jnp.sum(placed, axis=1, keepdims=True)

    def exchange(slot):
        for to in v_peers:
            pltpu.make_async_remote_copy(
                src_ref=comm.at[slot, my_v], dst_ref=comm.at[slot, my_v],
                send_sem=comm_ssem, recv_sem=comm_rsem.at[slot],
                device_id=(my_dp, to), device_id_type=MESH,
            ).start()

    def arrive(slot):
        others = comm.at[slot, pl.ds(0, vocab - 1)]
        pltpu.make_async_remote_copy(
            src_ref=others, dst_ref=others, send_sem=comm_ssem, recv_sem=comm_rsem.at[slot],
            device_id=(my_dp, v_peers[0]), device_id_type=MESH,
        ).wait_recv()

    def peak(n):
        wide = 2 * LANES
        running = [x[n, :, pl.ds(k * wide, wide)] for k in range(min(4, full // 2))]
        for k in range(4, full // 2):
            running[k % 4] = jnp.maximum(running[k % 4], x[n, :, pl.ds(k * wide, wide)])
        top = tree(jnp.maximum, running).astype(jnp.float32)
        top = jnp.maximum(top[:, :LANES], top[:, LANES:])
        if full % 2:
            top = jnp.maximum(top, x[n, :, pl.ds((full - 1) * LANES, LANES)].astype(jnp.float32))
        if tail:
            top = jnp.maximum(top, tail_tile(x, n, LOW))
        return jnp.max(top, axis=1, keepdims=True)

    def expo(n, top):
        parts = [zero] * 4
        for a, size in slabs(full, SLAB):
            raw = x[n, :, pl.ds(a * LANES, size * LANES)].astype(jnp.float32)
            value = jnp.exp(raw - top)
            e[n, :, pl.ds(a * LANES, size * LANES)] = value
            for k in range(size):
                parts[k % 4] = parts[k % 4] + value[:, k * LANES:(k + 1) * LANES]
        if tail:
            value = jnp.exp(tail_tile(x, n, LOW) - top)
            e[n, :, pl.ds(full * LANES, LANES)] = value
            parts[0] = parts[0] + value
        return jnp.sum((parts[0] + parts[1]) + (parts[2] + parts[3]), axis=1, keepdims=True)

    tops, sums = {}, {}

    def take(i):
        n, size = pairs[i]
        with scope(f"load{i}"):
            x_loads[i].wait()
            if i == 0:
                for load in d_loads:
                    load.start()
        with scope(f"peak{i}"):
            for m in range(n, n + size):
                tops[m] = peak(m)

    take(0)
    for i, (n, size) in enumerate(pairs):
        if i + 1 < len(pairs):
            take(i + 1)
        with scope(f"expo{i}"):
            for m in range(n, n + size):
                sums[m] = expo(m, tops[m])
    with scope("send1"):
        comm[0, my_v] = jnp.concatenate([to_row(tops), to_row(sums)], axis=0)
    with scope("barrier"):
        pl.semaphore_wait(barrier, vocab - 1 + groups - 1)
        exchange(0)

    with scope("pick"):
        column0 = my_v * width
        chosen, drafted = {}, {}
        for copy in scalars:
            copy.wait()
        pltpu.make_async_copy(d_hbm, d, d_sem).wait()
        for n in range(seqs):
            spot = jnp.zeros((depth, LANES), jnp.int32)
            for j in range(depth):
                spot = jnp.where(sub == j, tok[n, j], spot)
            spot = spot - column0 - lane
            hit_x, hit_d = zero, zero
            if tail:
                hit = (spot == full * LANES) & (lane < tail)
                hit_x = jnp.where(hit, tail_tile(x, n, 0.0), hit_x)
                hit_d = jnp.where(hit, tail_tile(d, n, 0.0), hit_d)
            for a, size in slabs(full, SLAB):
                columns = pl.ds(a * LANES, size * LANES)
                raw_x, raw_d = x[n, :, columns].astype(jnp.float32), d[n, :, columns].astype(jnp.float32)
                for k in range(size):
                    hit = spot == (a + k) * LANES
                    hit_x = jnp.where(hit, raw_x[:, k * LANES:(k + 1) * LANES], hit_x)
                    hit_d = jnp.where(hit, raw_d[:, k * LANES:(k + 1) * LANES], hit_d)
            chosen[n] = jnp.sum(hit_x, axis=1, keepdims=True)
            drafted[n] = jnp.sum(hit_d, axis=1, keepdims=True)
        comm[pick_slot, my_v] = jnp.concatenate([to_row(chosen), to_row(drafted)], axis=0)
        exchange(pick_slot)

    with scope("arrive1"):
        arrive(0)
    with scope("merge"):
        parts = [comm[0, p] for p in range(vocab)]
        peak_row = tree(jnp.maximum, [part[0:1] for part in parts])
        total_row = tree(jnp.add, [part[1:2] * jnp.exp(part[0:1] - peak_row) for part in parts])
        scale = jnp.exp(comm[0, my_v][0:1] - peak_row) / total_row
        scales = {n: to_column(scale, n) for n in range(seqs)}
    norms = {}
    for n in range(seqs):
        with scope(f"gap{n}"):
            upper = scales[n] * (1.0 + mixing)
            lower = scales[n] * mixing
            parts = [zero] * 4
            for a, size in slabs(full, SLAB):
                columns = pl.ds(a * LANES, size * LANES)
                value = e[n, :, columns]
                value = jnp.maximum(value * upper - d[n, :, columns].astype(jnp.float32), value * lower)
                e[n, :, columns] = value
                for k in range(size):
                    parts[k % 4] = parts[k % 4] + value[:, k * LANES:(k + 1) * LANES]
            if tail:
                value = e[n, :, pl.ds(full * LANES, LANES)]
                value = jnp.maximum(value * upper - tail_tile(d, n, 0.0), value * lower)
                e[n, :, pl.ds(full * LANES, LANES)] = value
                parts[0] = parts[0] + value
            norms[n] = jnp.sum((parts[0] + parts[1]) + (parts[2] + parts[3]), axis=1, keepdims=True)
    with scope("send2"):
        norm = to_row(norms)
        comm[norm_slot, my_v] = jnp.concatenate([norm, norm], axis=0)
        exchange(norm_slot)

    with scope("arrivep"):
        arrive(pick_slot)
    with scope("weights"):
        picked = tree(jnp.add, [comm[pick_slot, p] for p in range(vocab)])
        length_row = jnp.zeros((1, LANES), jnp.int32)
        places = []
        for n in range(seqs):
            rank = jnp.int32(0)
            for i in range(n):
                rank = rank + jnp.where(own[i] == own[n], 1, 0)
            places.append(own[n] * capacity + rank)
            length_row = jnp.where(lane_n == n, lens[n], length_row)
        live = lane_j < length_row
        safe_draft = jnp.where(live, picked[1:2], 1.0)
        accept = jnp.where(live, jnp.minimum(1.0, jnp.exp(picked[0:1] - peak_row) / total_row / safe_draft), 0.0)
        wide = jnp.broadcast_to(accept, (depth, LANES))
        before = tree(jnp.multiply, [
            jnp.where(lane_j >= k, pltpu.roll(wide, k, 1)[0:1], 1.0) for k in range(1, depth)
        ])
        weight = jnp.where(live, before * (1.0 - accept), 0.0)
        survive = before * accept
        inner = lax.broadcasted_iota(jnp.int32, (slots, TERMS * rows), 1)
        outer = lax.broadcasted_iota(jnp.int32, (slots, TERMS * rows), 0)
        picker = jnp.zeros((slots, TERMS * rows), jnp.float32)
        for n in range(seqs):
            picker = jnp.where((lax.rem(inner // depth, seqs) == n) & (outer == places[n]), 1.0, picker)
        picker = picker.astype(jnp.bfloat16)
    with scope("smallsend"):
        sent = zero
        for n in range(seqs):
            sent = jnp.where(lane == places[n], to_column(accept, n), sent)
            alive = jnp.where((lane_n == n) & (row_lane < rows), survive, 0.0)
            sent = jnp.where(lane == places[n] + half, jnp.sum(alive, axis=1, keepdims=True), sent)
        for g in range(groups):
            shift = (LANES - g * capacity) % LANES
            small[g] = pltpu.roll(sent, shift, 1) if shift else sent
        for to in g_peers:
            pltpu.make_async_remote_copy(
                src_ref=small.at[to], dst_ref=small_in.at[my_dp], send_sem=sm_ssem, recv_sem=sm_rsem,
                device_id=(to, my_v), device_id_type=MESH,
            ).start()
        small_in[my_dp] = small[my_dp]

    with scope("arrive2"):
        arrive(norm_slot)
    with scope("coef"):
        coef = weight / tree(jnp.add, [comm[norm_slot, p][0:1] for p in range(vocab)])
        coefs = [to_column(coef, n) for n in range(seqs)]

    bounds = plan(tiles)
    chunks = len(bounds) - 1

    def span(c):
        return pl.ds(bounds[c] * LANES, (bounds[c + 1] - bounds[c]) * LANES)

    for c in range(chunks):
        with scope(f"mix{c}"):
            for a, size in slabs(bounds[c + 1] - bounds[c], PIECE):
                columns = pl.ds((bounds[c] + a) * LANES, size * LANES)
                value = jnp.concatenate([e[n, :, columns] * coefs[n] for n in range(seqs)], axis=0)
                terms = []
                for _ in range(TERMS):
                    terms.append(value.astype(jnp.bfloat16))
                    value = value - terms[-1].astype(jnp.float32)
                mixed = jnp.dot(picker, jnp.concatenate(terms, axis=0), preferred_element_type=jnp.float32)
                for g in range(groups):
                    send[g, :, columns] = mixed[g * capacity:(g + 1) * capacity].astype(jnp.bfloat16)
            for to in g_peers:
                pltpu.make_async_remote_copy(
                    src_ref=send.at[to, :, span(c)], dst_ref=landed.at[my_dp, :, span(c)],
                    send_sem=out_ssem, recv_sem=out_rsem.at[c],
                    device_id=(to, my_v), device_id_type=MESH,
                ).start()
            landed[my_dp, :, span(c)] = send[my_dp, :, span(c)]

    with scope("smallrecv"):
        others = pl.ds(0, groups - 1)
        pltpu.make_async_remote_copy(
            src_ref=small.at[others], dst_ref=small_in.at[others], send_sem=sm_ssem, recv_sem=sm_rsem,
            device_id=(g_peers[0], my_v), device_id_type=MESH,
        ).wait()
        final = zero
        for g in range(groups):
            mine = lax.rem(lane, half) // capacity == g
            final = jnp.where(mine, pltpu.roll(small_in[g], g * capacity, 1), final)
        accept_out[...] = final[:, :slots]
        expected_out[...] = final[0:1, half:half + slots]

    for c in range(chunks):
        with scope(f"recv{c}"):
            pltpu.make_async_remote_copy(
                src_ref=send.at[others, :, span(c)], dst_ref=landed.at[others, :, span(c)],
                send_sem=out_ssem, recv_sem=out_rsem.at[c],
                device_id=(g_peers[0], my_v), device_id_type=MESH,
            ).wait_recv()
        with scope(f"gather{c}"):
            for a, size in slabs(bounds[c + 1] - bounds[c], SLAB):
                start = (bounds[c] + a) * LANES
                columns = pl.ds(start, size * LANES)
                pieces = [landed[g, :, columns].astype(jnp.float32) for g in range(groups)]
                whole = jnp.concatenate(pieces, axis=0).astype(jnp.bfloat16)
                kept = min(size * LANES, width - start)
                block[:, pl.ds(start, kept)] = whole[:, :kept]
    with scope("sendwait"):
        pltpu.make_async_remote_copy(
            src_ref=send.at[others], dst_ref=landed.at[others], send_sem=out_ssem, recv_sem=out_rsem.at[0],
            device_id=(g_peers[0], my_v), device_id_type=MESH,
        ).wait_send()
        others = comm.at[:, pl.ds(0, vocab - 1)]
        pltpu.make_async_remote_copy(
            src_ref=others, dst_ref=others, send_sem=comm_ssem, recv_sem=comm_rsem.at[0],
            device_id=(my_dp, v_peers[0]), device_id_type=MESH,
        ).wait_send()


def finish(block, accept, expected, out, accept_out, expected_out, sem):
    pairs = ((block, out), (accept, accept_out), (expected, expected_out))
    copies = [pltpu.make_async_copy(a, b, sem.at[i]) for i, (a, b) in enumerate(pairs)]
    for copy in copies:
        copy.start()
    for copy in copies:
        copy.wait()


def body(logits, draft_probs, draft_tokens, draft_lengths, owner_group):
    groups = lax.axis_size("dp")
    vocab = lax.axis_size("vocab")
    seqs, depth, width = logits.shape
    capacity = max(2, 2 * seqs // groups)
    tiles = -(-width // LANES)
    padded = tiles * LANES
    chunks = len(plan(tiles)) - 1
    hbm = pl.BlockSpec(memory_space=pltpu.HBM)
    vmem = pl.BlockSpec(memory_space=pltpu.VMEM)
    dma = pltpu.SemaphoreType.DMA
    slots = groups * capacity
    shapes = (
        jax.ShapeDtypeStruct((slots, width), jnp.bfloat16),
        jax.ShapeDtypeStruct((depth, slots), jnp.float32),
        jax.ShapeDtypeStruct((1, slots), jnp.float32),
    )
    outs = pl.pallas_call(
        functools.partial(kernel, (groups, vocab, capacity)),
        out_shape=shapes,
        in_specs=[hbm] * 5,
        out_specs=(vmem, vmem, vmem),
        scratch_shapes=[
            pltpu.SMEM((seqs, depth), jnp.int32),
            pltpu.SMEM((seqs,), jnp.int32),
            pltpu.SMEM((seqs,), jnp.int32),
            pltpu.VMEM((seqs, depth, width), jnp.bfloat16),
            pltpu.VMEM((seqs, depth, width), jnp.bfloat16),
            pltpu.VMEM((seqs, depth, padded), jnp.float32),
            pltpu.VMEM((groups, capacity, padded), jnp.bfloat16),
            pltpu.VMEM((groups, capacity, padded), jnp.bfloat16),
            pltpu.VMEM((BATCHES + 2, vocab, 2, LANES), jnp.float32),
            pltpu.VMEM((groups, depth, LANES), jnp.float32),
            pltpu.VMEM((groups, depth, LANES), jnp.float32),
            dma((3,)),
            dma((len(slabs(seqs, PAIR)),)),
            dma(()),
            dma(()),
            dma((BATCHES + 2,)),
            dma(()),
            dma((chunks,)),
            dma(()),
            dma(()),
        ],
        compiler_params=pltpu.CompilerParams(
            collective_id=0, has_side_effects=True, vmem_limit_bytes=54500 * 1024
        ),
    )(*[pltpu.with_memory_space_constraint(a, pltpu.HBM) for a in (draft_tokens, draft_lengths, owner_group)], logits, draft_probs)
    out, accept, expected = pl.pallas_call(
        finish,
        out_shape=shapes,
        in_specs=[vmem] * 3,
        out_specs=(hbm, hbm, hbm),
        scratch_shapes=[dma((3,))],
        compiler_params=pltpu.CompilerParams(vmem_limit_bytes=1024 * 1024),
    )(*outs)
    return (out, accept.T, expected.reshape(slots))


def solution(mesh):
    placed = (P("dp", None, "vocab"), P("dp", None, "vocab"), P("dp", None), P("dp"), P("dp"))
    return jax.shard_map(
        body,
        mesh=mesh,
        in_specs=placed,
        out_specs=(P("dp", "vocab"), P("dp", None), P("dp")),
        check_vma=False,
    )
```

```python
import functools

import jax
import jax.numpy as jnp
from jax import lax
from jax.experimental import pallas as pl
from jax.experimental.pallas import tpu as pltpu
from jax.sharding import PartitionSpec as P

mixing = 0.1
LANES = 128
SLAB = 8
PIECE = 2
BATCHES = 1
TERMS = 3
PARTS = 1
PAIR = 2
FIRST = 4
GROWTH = 3
MOST = 40
LOW = -1e30
MESH = pl.DeviceIdType.MESH
scope = jax.named_scope


def slabs(full, size):
    return [(a, min(size, full - a)) for a in range(0, full, size)]


def plan(tiles):
    bounds, size = [0], FIRST
    while bounds[-1] < tiles:
        bounds.append(min(tiles, bounds[-1] + size))
        size = min(size * GROWTH, MOST)
    return bounds


def xor(value, mask):
    bit = 1
    while bit <= mask:
        if mask & bit:
            value = value + bit - 2 * bit * lax.rem(value // bit, 2)
        bit *= 2
    return value


def partners(me, count):
    if count & (count - 1):
        return [lax.rem(me + k, count) for k in range(1, count)]
    return [xor(me, k) for k in range(count - 1, 0, -1)]


def by_distance(me, count):
    picks = [jnp.where(2 * me < count, count - 2 - i, i) for i in range(count - 1)]
    return [p + jnp.where(p >= me, 1, 0) for p in picks]


def tree(op, values):
    values = list(values)
    while len(values) > 1:
        values = [op(*values[i:i + 2]) if i + 1 < len(values) else values[i] for i in range(0, len(values), 2)]
    return values[0]


def kernel(
    dims,
    tok_hbm, lens_hbm, own_hbm, x_hbm, d_hbm,
    block, accept_out, expected_out,
    tok, lens, own, x, d, e, send, landed, comm, small, small_in,
    scalar_sem, x_sem, d_sem, comm_ssem, comm_rsem, out_ssem, out_rsem, sm_ssem, sm_rsem,
):
    groups, vocab, capacity = dims
    seqs, depth, width = x_hbm.shape
    full = width // LANES
    tail = width - full * LANES
    tiles = e.shape[2] // LANES
    rows = seqs * depth
    slots = groups * capacity
    half = LANES // 2
    pick_slot, norm_slot = BATCHES, BATCHES + 1
    my_dp = lax.axis_index("dp")
    my_v = lax.axis_index("vocab")

    barrier = pltpu.get_barrier_semaphore()
    v_peers = by_distance(my_v, vocab)
    g_peers = partners(my_dp, groups)
    for p in v_peers:
        pl.semaphore_signal(barrier, inc=1, device_id=(my_dp, p), device_id_type=MESH)
    for p in g_peers:
        pl.semaphore_signal(barrier, inc=1, device_id=(p, my_v), device_id_type=MESH)

    pairs = slabs(seqs, PAIR)
    x_loads, d_loads = [], []
    for i, (n, size) in enumerate(pairs):
        part = pl.ds(n, size)
        x_loads.append(pltpu.make_async_copy(x_hbm.at[part], x.at[part], x_sem.at[i]))
        d_loads.append(pltpu.make_async_copy(d_hbm.at[part], d.at[part], d_sem))
        x_loads[-1].start()
    scalars = []
    for i, (source, target) in enumerate(((tok_hbm, tok), (lens_hbm, lens), (own_hbm, own))):
        scalars.append(pltpu.make_async_copy(source, target, scalar_sem.at[i]))
        scalars[-1].start()

    sub = lax.broadcasted_iota(jnp.int32, (depth, LANES), 0)
    lane = lax.broadcasted_iota(jnp.int32, (depth, LANES), 1)
    row_lane = lax.broadcasted_iota(jnp.int32, (1, LANES), 1)
    lane_j = lax.rem(row_lane, depth)
    lane_n = lax.rem(row_lane // depth, seqs)
    zero = jnp.zeros((depth, LANES), jnp.float32)
    spots = [(lax.rem(lane, depth) == sub) & (lax.rem(lane // depth, seqs) == n) for n in range(seqs)]

    def tail_tile(ref, n, fill):
        part = ref[n, :, pl.ds(full * LANES, tail)].astype(jnp.float32)
        return jnp.concatenate([part, jnp.full((depth, LANES - tail), fill, jnp.float32)], axis=1)

    def to_row(columns):
        spread = zero
        for n, column in columns.items():
            spread = jnp.where(spots[n], column, spread)
        return jnp.sum(spread, axis=0, keepdims=True)

    def to_column(row, n):
        placed = jnp.where(spots[n] & (lane < rows), row, 0.0)
        return jnp.sum(placed, axis=1, keepdims=True)

    def exchange(slot):
        for to in v_peers:
            pltpu.make_async_remote_copy(
                src_ref=comm.at[slot, my_v], dst_ref=comm.at[slot, my_v],
                send_sem=comm_ssem, recv_sem=comm_rsem.at[slot],
                device_id=(my_dp, to), device_id_type=MESH,
            ).start()

    def arrive(slot):
        others = comm.at[slot, pl.ds(0, vocab - 1)]
        pltpu.make_async_remote_copy(
            src_ref=others, dst_ref=others, send_sem=comm_ssem, recv_sem=comm_rsem.at[slot],
            device_id=(my_dp, v_peers[0]), device_id_type=MESH,
        ).wait_recv()

    def peak(n):
        wide = 2 * LANES
        running = [x[n, :, pl.ds(k * wide, wide)] for k in range(min(4, full // 2))]
        for k in range(4, full // 2):
            running[k % 4] = jnp.maximum(running[k % 4], x[n, :, pl.ds(k * wide, wide)])
        top = tree(jnp.maximum, running).astype(jnp.float32)
        top = jnp.maximum(top[:, :LANES], top[:, LANES:])
        if full % 2:
            top = jnp.maximum(top, x[n, :, pl.ds((full - 1) * LANES, LANES)].astype(jnp.float32))
        if tail:
            top = jnp.maximum(top, tail_tile(x, n, LOW))
        return jnp.max(top, axis=1, keepdims=True)

    def expo(n, top):
        parts = [zero] * 4
        for a, size in slabs(full, SLAB):
            raw = x[n, :, pl.ds(a * LANES, size * LANES)].astype(jnp.float32)
            value = jnp.exp(raw - top)
            e[n, :, pl.ds(a * LANES, size * LANES)] = value
            for k in range(size):
                parts[k % 4] = parts[k % 4] + value[:, k * LANES:(k + 1) * LANES]
        if tail:
            value = jnp.exp(tail_tile(x, n, LOW) - top)
            e[n, :, pl.ds(full * LANES, LANES)] = value
            parts[0] = parts[0] + value
        return jnp.sum((parts[0] + parts[1]) + (parts[2] + parts[3]), axis=1, keepdims=True)

    tops, sums = {}, {}

    def take(i):
        n, size = pairs[i]
        with scope(f"load{i}"):
            x_loads[i].wait()
            if i == 0:
                for load in d_loads:
                    load.start()
        with scope(f"peak{i}"):
            for m in range(n, n + size):
                tops[m] = peak(m)

    take(0)
    for i, (n, size) in enumerate(pairs):
        if i + 1 < len(pairs):
            take(i + 1)
        with scope(f"expo{i}"):
            for m in range(n, n + size):
                sums[m] = expo(m, tops[m])
    with scope("send1"):
        comm[0, my_v] = jnp.concatenate([to_row(tops), to_row(sums)], axis=0)
    with scope("barrier"):
        pl.semaphore_wait(barrier, vocab - 1 + groups - 1)
        exchange(0)

    with scope("pick"):
        column0 = my_v * width
        chosen, drafted, masses = {}, {}, {}
        for copy in scalars:
            copy.wait()
        pltpu.make_async_copy(d_hbm, d, d_sem).wait()
        for n in range(seqs):
            spot = jnp.zeros((depth, LANES), jnp.int32)
            for j in range(depth):
                spot = jnp.where(sub == j, tok[n, j], spot)
            spot = spot - column0 - lane
            hit_x, hit_d, mass = zero, zero, [zero] * 4
            if tail:
                hit = (spot == full * LANES) & (lane < tail)
                hit_x = jnp.where(hit, tail_tile(x, n, 0.0), hit_x)
                hit_d = jnp.where(hit, tail_tile(d, n, 0.0), hit_d)
                mass[0] = tail_tile(d, n, 0.0)
            for a, size in slabs(full, SLAB):
                columns = pl.ds(a * LANES, size * LANES)
                raw_x, raw_d = x[n, :, columns].astype(jnp.float32), d[n, :, columns].astype(jnp.float32)
                for k in range(size):
                    hit = spot == (a + k) * LANES
                    hit_x = jnp.where(hit, raw_x[:, k * LANES:(k + 1) * LANES], hit_x)
                    hit_d = jnp.where(hit, raw_d[:, k * LANES:(k + 1) * LANES], hit_d)
                    mass[k % 4] = mass[k % 4] + raw_d[:, k * LANES:(k + 1) * LANES]
            chosen[n] = jnp.sum(hit_x, axis=1, keepdims=True)
            drafted[n] = jnp.sum(hit_d, axis=1, keepdims=True)
            masses[n] = (mass[0] + mass[1]) + (mass[2] + mass[3])
        comm[pick_slot, my_v] = jnp.concatenate([to_row(chosen), to_row(drafted)], axis=0)
        exchange(pick_slot)

    with scope("arrive1"):
        arrive(0)
    with scope("merge"):
        parts = [comm[0, p] for p in range(vocab)]
        peak_row = tree(jnp.maximum, [part[0:1] for part in parts])
        total_row = tree(jnp.add, [part[1:2] * jnp.exp(part[0:1] - peak_row) for part in parts])
        mine = comm[0, my_v]
        scale = jnp.exp(mine[0:1] - peak_row) / total_row
        scales = [to_column(scale, n) for n in range(seqs)]
    excess = {}
    for n in range(seqs):
        with scope(f"gap{n}"):
            parts = [zero] * 4
            for a, size in slabs(full, SLAB):
                columns = pl.ds(a * LANES, size * LANES)
                upper = jnp.maximum(e[n, :, columns] * scales[n], d[n, :, columns].astype(jnp.float32))
                for k in range(size):
                    parts[k % 4] = parts[k % 4] + upper[:, k * LANES:(k + 1) * LANES]
            if tail:
                parts[0] = parts[0] + jnp.maximum(e[n, :, pl.ds(full * LANES, LANES)] * scales[n], tail_tile(d, n, 0.0))
            total = (parts[0] + parts[1]) + (parts[2] + parts[3])
            excess[n] = jnp.sum(total - masses[n], axis=1, keepdims=True)
    with scope("send2"):
        norm = to_row(excess) + mixing * scale * mine[1:2]
        comm[norm_slot, my_v] = jnp.concatenate([norm, norm], axis=0)
        exchange(norm_slot)

    with scope("arrivep"):
        arrive(pick_slot)
    with scope("weights"):
        picked = tree(jnp.add, [comm[pick_slot, p] for p in range(vocab)])
        length_row = jnp.zeros((1, LANES), jnp.int32)
        places = []
        for n in range(seqs):
            rank = jnp.int32(0)
            for i in range(n):
                rank = rank + jnp.where(own[i] == own[n], 1, 0)
            places.append(own[n] * capacity + rank)
            length_row = jnp.where(lane_n == n, lens[n], length_row)
        live = lane_j < length_row
        safe_draft = jnp.where(live, picked[1:2], 1.0)
        accept = jnp.where(live, jnp.minimum(1.0, jnp.exp(picked[0:1] - peak_row) / total_row / safe_draft), 0.0)
        wide = jnp.broadcast_to(accept, (depth, LANES))
        before = tree(jnp.multiply, [
            jnp.where(lane_j >= k, pltpu.roll(wide, k, 1)[0:1], 1.0) for k in range(1, depth)
        ])
        weight = jnp.where(live, before * (1.0 - accept), 0.0)
        survive = before * accept
        inner = lax.broadcasted_iota(jnp.int32, (slots, TERMS * rows), 1)
        outer = lax.broadcasted_iota(jnp.int32, (slots, TERMS * rows), 0)
        picker = jnp.zeros((slots, TERMS * rows), jnp.float32)
        for n in range(seqs):
            picker = jnp.where((lax.rem(inner // depth, seqs) == n) & (outer == places[n]), 1.0, picker)
        picker = picker.astype(jnp.bfloat16)
    with scope("smallsend"):
        sent = zero
        for n in range(seqs):
            sent = jnp.where(lane == places[n], to_column(accept, n), sent)
            alive = jnp.where((lane_n == n) & (row_lane < rows), survive, 0.0)
            sent = jnp.where(lane == places[n] + half, jnp.sum(alive, axis=1, keepdims=True), sent)
        for g in range(groups):
            shift = (LANES - g * capacity) % LANES
            small[g] = pltpu.roll(sent, shift, 1) if shift else sent
        for to in g_peers:
            pltpu.make_async_remote_copy(
                src_ref=small.at[to], dst_ref=small_in.at[my_dp], send_sem=sm_ssem, recv_sem=sm_rsem,
                device_id=(to, my_v), device_id_type=MESH,
            ).start()
        small_in[my_dp] = small[my_dp]

    with scope("arrive2"):
        arrive(norm_slot)
    with scope("coef"):
        coef = weight / tree(jnp.add, [comm[norm_slot, p][0:1] for p in range(vocab)])
        coefs = [to_column(coef, n) for n in range(seqs)]
        lowers = [to_column(coef * scale * mixing, n) for n in range(seqs)]
        uppers = [to_column(coef * scale * (1.0 + mixing), n) for n in range(seqs)]

    bounds = plan(tiles)
    chunks = len(bounds) - 1

    def pieces(c):
        whole = min(bounds[c + 1], full)
        found = [(bounds[c] + a, size) for a, size in slabs(whole - bounds[c], PIECE)]
        return found + ([(full, 1)] if bounds[c + 1] > full else [])

    def span(c):
        return pl.ds(bounds[c] * LANES, (bounds[c + 1] - bounds[c]) * LANES)

    square = groups == 4
    near, far, across = xor(my_dp, 1), xor(my_dp, 2), xor(my_dp, 3)

    def ship(c, to):
        pltpu.make_async_remote_copy(
            src_ref=send.at[to, :, span(c)], dst_ref=landed.at[my_dp, :, span(c)],
            send_sem=out_ssem, recv_sem=out_rsem.at[c],
            device_id=(to, my_v), device_id_type=MESH,
        ).start()

    for c in range(chunks):
        with scope(f"mix{c}"):
            for start, size in pieces(c):
                columns = pl.ds(start * LANES, size * LANES)
                values = []
                for n in range(seqs):
                    value = e[n, :, columns]
                    draft = tail_tile(d, n, 0.0) if start >= full else d[n, :, columns].astype(jnp.float32)
                    values.append(jnp.maximum(value * uppers[n] - draft * coefs[n], value * lowers[n]))
                value = jnp.concatenate(values, axis=0)
                terms = []
                for _ in range(TERMS):
                    terms.append(value.astype(jnp.bfloat16))
                    value = value - terms[-1].astype(jnp.float32)
                mixed = jnp.dot(picker, jnp.concatenate(terms, axis=0), preferred_element_type=jnp.float32)
                for g in range(groups):
                    send[g, :, columns] = mixed[g * capacity:(g + 1) * capacity].astype(jnp.bfloat16)
            if square:
                ship(c, far)

                @pl.when(across < near)
                def _():
                    ship(c, across)

                @pl.when(jnp.logical_not(across < near))
                def _():
                    ship(c, near)
            else:
                for to in g_peers:
                    ship(c, to)
            landed[my_dp, :, span(c)] = send[my_dp, :, span(c)]

    if square:
        @pl.when(across < near)
        def _():
            for c in range(chunks):
                ship(c, near)

        @pl.when(jnp.logical_not(across < near))
        def _():
            for c in range(chunks):
                ship(c, across)

    with scope("smallrecv"):
        others = pl.ds(0, groups - 1)
        pltpu.make_async_remote_copy(
            src_ref=small.at[others], dst_ref=small_in.at[others], send_sem=sm_ssem, recv_sem=sm_rsem,
            device_id=(g_peers[0], my_v), device_id_type=MESH,
        ).wait()
        final = zero
        for g in range(groups):
            mine = lax.rem(lane, half) // capacity == g
            final = jnp.where(mine, pltpu.roll(small_in[g], g * capacity, 1), final)
        accept_out[...] = final[:, :slots]
        expected_out[...] = final[0:1, half:half + slots]

    for c in range(chunks):
        with scope(f"recv{c}"):
            pltpu.make_async_remote_copy(
                src_ref=send.at[others, :, span(c)], dst_ref=landed.at[others, :, span(c)],
                send_sem=out_ssem, recv_sem=out_rsem.at[c],
                device_id=(g_peers[0], my_v), device_id_type=MESH,
            ).wait_recv()
        with scope(f"gather{c}"):
            for a, size in slabs(bounds[c + 1] - bounds[c], SLAB):
                start = (bounds[c] + a) * LANES
                columns = pl.ds(start, size * LANES)
                pieces = [landed[g, :, columns].astype(jnp.float32) for g in range(groups)]
                whole = jnp.concatenate(pieces, axis=0).astype(jnp.bfloat16)
                kept = min(size * LANES, width - start)
                block[:, pl.ds(start, kept)] = whole[:, :kept]
    with scope("sendwait"):
        pltpu.make_async_remote_copy(
            src_ref=send.at[others], dst_ref=landed.at[others], send_sem=out_ssem, recv_sem=out_rsem.at[0],
            device_id=(g_peers[0], my_v), device_id_type=MESH,
        ).wait_send()
        others = comm.at[:, pl.ds(0, vocab - 1)]
        pltpu.make_async_remote_copy(
            src_ref=others, dst_ref=others, send_sem=comm_ssem, recv_sem=comm_rsem.at[0],
            device_id=(my_dp, v_peers[0]), device_id_type=MESH,
        ).wait_send()


def finish(block, accept, expected, out, accept_out, expected_out, sem):
    step = -(-block.shape[1] // (PARTS * LANES)) * LANES
    spans = [pl.ds(a, min(step, block.shape[1] - a)) for a in range(0, block.shape[1], step)]
    pairs = [(block.at[:, c], out.at[:, c]) for c in spans] + [(accept, accept_out), (expected, expected_out)]
    copies = [pltpu.make_async_copy(a, b, sem.at[i]) for i, (a, b) in enumerate(pairs)]
    for copy in copies:
        copy.start()
    for copy in copies:
        copy.wait()


def body(logits, draft_probs, draft_tokens, draft_lengths, owner_group):
    groups = lax.axis_size("dp")
    vocab = lax.axis_size("vocab")
    seqs, depth, width = logits.shape
    capacity = max(2, 2 * seqs // groups)
    tiles = -(-width // LANES)
    padded = tiles * LANES
    chunks = len(plan(tiles)) - 1
    hbm = pl.BlockSpec(memory_space=pltpu.HBM)
    vmem = pl.BlockSpec(memory_space=pltpu.VMEM)
    dma = pltpu.SemaphoreType.DMA
    slots = groups * capacity
    shapes = (
        jax.ShapeDtypeStruct((slots, width), jnp.bfloat16),
        jax.ShapeDtypeStruct((depth, slots), jnp.float32),
        jax.ShapeDtypeStruct((1, slots), jnp.float32),
    )
    outs = pl.pallas_call(
        functools.partial(kernel, (groups, vocab, capacity)),
        out_shape=shapes,
        in_specs=[hbm] * 5,
        out_specs=(vmem, vmem, vmem),
        scratch_shapes=[
            pltpu.SMEM((seqs, depth), jnp.int32),
            pltpu.SMEM((seqs,), jnp.int32),
            pltpu.SMEM((seqs,), jnp.int32),
            pltpu.VMEM((seqs, depth, width), jnp.bfloat16),
            pltpu.VMEM((seqs, depth, width), jnp.bfloat16),
            pltpu.VMEM((seqs, depth, padded), jnp.float32),
            pltpu.VMEM((groups, capacity, padded), jnp.bfloat16),
            pltpu.VMEM((groups, capacity, padded), jnp.bfloat16),
            pltpu.VMEM((BATCHES + 2, vocab, 2, LANES), jnp.float32),
            pltpu.VMEM((groups, depth, LANES), jnp.float32),
            pltpu.VMEM((groups, depth, LANES), jnp.float32),
            dma((3,)),
            dma((len(slabs(seqs, PAIR)),)),
            dma(()),
            dma(()),
            dma((BATCHES + 2,)),
            dma(()),
            dma((chunks,)),
            dma(()),
            dma(()),
        ],
        compiler_params=pltpu.CompilerParams(
            collective_id=0, has_side_effects=True, vmem_limit_bytes=54500 * 1024
        ),
    )(*[pltpu.with_memory_space_constraint(a, pltpu.HBM) for a in (draft_tokens, draft_lengths, owner_group)], logits, draft_probs)
    out, accept, expected = pl.pallas_call(
        finish,
        out_shape=shapes,
        in_specs=[vmem] * 3,
        out_specs=(hbm, hbm, hbm),
        scratch_shapes=[dma((PARTS + 2,))],
        compiler_params=pltpu.CompilerParams(vmem_limit_bytes=1024 * 1024),
    )(*outs)
    return (out, accept.T, expected.reshape(slots))


def solution(mesh):
    placed = (P("dp", None, "vocab"), P("dp", None, "vocab"), P("dp", None), P("dp"), P("dp"))
    return jax.shard_map(
        body,
        mesh=mesh,
        in_specs=placed,
        out_specs=(P("dp", "vocab"), P("dp", None), P("dp")),
        check_vma=False,
    )
```

```python
import functools

import jax
import jax.numpy as jnp
from jax import lax
from jax.experimental import pallas as pl
from jax.experimental.pallas import tpu as pltpu
from jax.sharding import PartitionSpec as P

mixing = 0.1
LANES = 128
SLAB = 8
PIECE = 2
BATCHES = 1
TERMS = 3
PARTS = 1
PAIR = 2
FIRST = 2
GROWTH = 3
MOST = 24
LOW = -1e30
MESH = pl.DeviceIdType.MESH
scope = jax.named_scope


def slabs(full, size):
    return [(a, min(size, full - a)) for a in range(0, full, size)]


def plan(tiles):
    bounds, size = [0], FIRST
    while bounds[-1] < tiles:
        bounds.append(min(tiles, bounds[-1] + size))
        size = min(size * GROWTH, MOST)
    return bounds


def xor(value, mask):
    bit = 1
    while bit <= mask:
        if mask & bit:
            value = value + bit - 2 * bit * lax.rem(value // bit, 2)
        bit *= 2
    return value


def partners(me, count):
    if count & (count - 1):
        return [lax.rem(me + k, count) for k in range(1, count)]
    return [xor(me, k) for k in range(count - 1, 0, -1)]


def by_distance(me, count):
    picks = [jnp.where(2 * me < count, count - 2 - i, i) for i in range(count - 1)]
    return [p + jnp.where(p >= me, 1, 0) for p in picks]


def tree(op, values):
    values = list(values)
    while len(values) > 1:
        values = [op(*values[i:i + 2]) if i + 1 < len(values) else values[i] for i in range(0, len(values), 2)]
    return values[0]


def kernel(
    dims,
    tok_hbm, lens_hbm, own_hbm, x_hbm, d_hbm,
    block, accept_out, expected_out,
    tok, lens, own, x, d, e, send, landed, comm, small, small_in,
    scalar_sem, x_sem, d_sem, comm_ssem, comm_rsem, out_ssem, out_rsem, sm_ssem, sm_rsem,
):
    groups, vocab, capacity = dims
    seqs, depth, width = x_hbm.shape
    full = width // LANES
    tail = width - full * LANES
    tiles = e.shape[2] // LANES
    rows = seqs * depth
    slots = groups * capacity
    half = LANES // 2
    pick_slot, norm_slot = BATCHES, BATCHES + 1
    my_dp = lax.axis_index("dp")
    my_v = lax.axis_index("vocab")

    barrier = pltpu.get_barrier_semaphore()
    v_peers = by_distance(my_v, vocab)
    g_peers = partners(my_dp, groups)
    for p in v_peers:
        pl.semaphore_signal(barrier, inc=1, device_id=(my_dp, p), device_id_type=MESH)
    for p in g_peers:
        pl.semaphore_signal(barrier, inc=1, device_id=(p, my_v), device_id_type=MESH)

    pairs = slabs(seqs, PAIR)
    x_loads, d_loads = [], []
    for i, (n, size) in enumerate(pairs):
        part = pl.ds(n, size)
        x_loads.append(pltpu.make_async_copy(x_hbm.at[part], x.at[part], x_sem.at[i]))
        d_loads.append(pltpu.make_async_copy(d_hbm.at[part], d.at[part], d_sem))
        x_loads[-1].start()
    scalars = []
    for i, (source, target) in enumerate(((tok_hbm, tok), (lens_hbm, lens), (own_hbm, own))):
        scalars.append(pltpu.make_async_copy(source, target, scalar_sem.at[i]))
        scalars[-1].start()

    sub = lax.broadcasted_iota(jnp.int32, (depth, LANES), 0)
    lane = lax.broadcasted_iota(jnp.int32, (depth, LANES), 1)
    row_lane = lax.broadcasted_iota(jnp.int32, (1, LANES), 1)
    lane_j = lax.rem(row_lane, depth)
    lane_n = lax.rem(row_lane // depth, seqs)
    zero = jnp.zeros((depth, LANES), jnp.float32)
    spots = [(lax.rem(lane, depth) == sub) & (lax.rem(lane // depth, seqs) == n) for n in range(seqs)]

    def tail_tile(ref, n, fill):
        part = ref[n, :, pl.ds(full * LANES, tail)].astype(jnp.float32)
        return jnp.concatenate([part, jnp.full((depth, LANES - tail), fill, jnp.float32)], axis=1)

    def to_row(columns):
        spread = zero
        for n, column in columns.items():
            spread = jnp.where(spots[n], column, spread)
        return jnp.sum(spread, axis=0, keepdims=True)

    def to_column(row, n):
        placed = jnp.where(spots[n] & (lane < rows), row, 0.0)
        return jnp.sum(placed, axis=1, keepdims=True)

    def exchange(slot):
        for to in v_peers:
            pltpu.make_async_remote_copy(
                src_ref=comm.at[slot, my_v], dst_ref=comm.at[slot, my_v],
                send_sem=comm_ssem, recv_sem=comm_rsem.at[slot],
                device_id=(my_dp, to), device_id_type=MESH,
            ).start()

    def arrive(slot):
        others = comm.at[slot, pl.ds(0, vocab - 1)]
        pltpu.make_async_remote_copy(
            src_ref=others, dst_ref=others, send_sem=comm_ssem, recv_sem=comm_rsem.at[slot],
            device_id=(my_dp, v_peers[0]), device_id_type=MESH,
        ).wait_recv()

    def peak(n):
        wide = 2 * LANES
        running = [x[n, :, pl.ds(k * wide, wide)] for k in range(min(4, full // 2))]
        for k in range(4, full // 2):
            running[k % 4] = jnp.maximum(running[k % 4], x[n, :, pl.ds(k * wide, wide)])
        top = tree(jnp.maximum, running).astype(jnp.float32)
        top = jnp.maximum(top[:, :LANES], top[:, LANES:])
        if full % 2:
            top = jnp.maximum(top, x[n, :, pl.ds((full - 1) * LANES, LANES)].astype(jnp.float32))
        if tail:
            top = jnp.maximum(top, tail_tile(x, n, LOW))
        return jnp.max(top, axis=1, keepdims=True)

    def expo(n, top):
        parts = [zero] * 4
        for a, size in slabs(full, SLAB):
            raw = x[n, :, pl.ds(a * LANES, size * LANES)].astype(jnp.float32)
            value = jnp.exp(raw - top)
            e[n, :, pl.ds(a * LANES, size * LANES)] = value
            for k in range(size):
                parts[k % 4] = parts[k % 4] + value[:, k * LANES:(k + 1) * LANES]
        if tail:
            value = jnp.exp(tail_tile(x, n, LOW) - top)
            e[n, :, pl.ds(full * LANES, LANES)] = value
            parts[0] = parts[0] + value
        return jnp.sum((parts[0] + parts[1]) + (parts[2] + parts[3]), axis=1, keepdims=True)

    tops, sums = {}, {}

    def take(i):
        n, size = pairs[i]
        with scope(f"load{i}"):
            x_loads[i].wait()
            if i == 0:
                for load in d_loads:
                    load.start()
        with scope(f"peak{i}"):
            for m in range(n, n + size):
                tops[m] = peak(m)

    take(0)
    for i, (n, size) in enumerate(pairs):
        if i + 1 < len(pairs):
            take(i + 1)
        with scope(f"expo{i}"):
            for m in range(n, n + size):
                sums[m] = expo(m, tops[m])
    with scope("send1"):
        comm[0, my_v] = jnp.concatenate([to_row(tops), to_row(sums)], axis=0)
    with scope("barrier"):
        pl.semaphore_wait(barrier, vocab - 1 + groups - 1)
        exchange(0)

    with scope("pick"):
        column0 = my_v * width
        chosen, drafted, masses = {}, {}, {}
        for copy in scalars:
            copy.wait()
        pltpu.make_async_copy(d_hbm, d, d_sem).wait()
        for n in range(seqs):
            spot = jnp.zeros((depth, LANES), jnp.int32)
            for j in range(depth):
                spot = jnp.where(sub == j, tok[n, j], spot)
            spot = spot - column0 - lane
            hit_x, hit_d, mass = zero, zero, [zero] * 4
            if tail:
                hit = (spot == full * LANES) & (lane < tail)
                hit_x = jnp.where(hit, tail_tile(x, n, 0.0), hit_x)
                hit_d = jnp.where(hit, tail_tile(d, n, 0.0), hit_d)
                mass[0] = tail_tile(d, n, 0.0)
            for a, size in slabs(full, SLAB):
                columns = pl.ds(a * LANES, size * LANES)
                raw_x, raw_d = x[n, :, columns].astype(jnp.float32), d[n, :, columns].astype(jnp.float32)
                for k in range(size):
                    hit = spot == (a + k) * LANES
                    hit_x = jnp.where(hit, raw_x[:, k * LANES:(k + 1) * LANES], hit_x)
                    hit_d = jnp.where(hit, raw_d[:, k * LANES:(k + 1) * LANES], hit_d)
                    mass[k % 4] = mass[k % 4] + raw_d[:, k * LANES:(k + 1) * LANES]
            chosen[n] = jnp.sum(hit_x, axis=1, keepdims=True)
            drafted[n] = jnp.sum(hit_d, axis=1, keepdims=True)
            masses[n] = (mass[0] + mass[1]) + (mass[2] + mass[3])
        comm[pick_slot, my_v] = jnp.concatenate([to_row(chosen), to_row(drafted)], axis=0)
        exchange(pick_slot)

    with scope("arrive1"):
        arrive(0)
    with scope("merge"):
        parts = [comm[0, p] for p in range(vocab)]
        peak_row = tree(jnp.maximum, [part[0:1] for part in parts])
        total_row = tree(jnp.add, [part[1:2] * jnp.exp(part[0:1] - peak_row) for part in parts])
        mine = comm[0, my_v]
        scale = jnp.exp(mine[0:1] - peak_row) / total_row
        scales = [to_column(scale, n) for n in range(seqs)]
    excess = {}
    for n in range(seqs):
        with scope(f"gap{n}"):
            parts = [zero] * 4
            for a, size in slabs(full, SLAB):
                columns = pl.ds(a * LANES, size * LANES)
                upper = jnp.maximum(e[n, :, columns] * scales[n], d[n, :, columns].astype(jnp.float32))
                for k in range(size):
                    parts[k % 4] = parts[k % 4] + upper[:, k * LANES:(k + 1) * LANES]
            if tail:
                parts[0] = parts[0] + jnp.maximum(e[n, :, pl.ds(full * LANES, LANES)] * scales[n], tail_tile(d, n, 0.0))
            total = (parts[0] + parts[1]) + (parts[2] + parts[3])
            excess[n] = jnp.sum(total - masses[n], axis=1, keepdims=True)
    with scope("send2"):
        norm = to_row(excess) + mixing * scale * mine[1:2]
        comm[norm_slot, my_v] = jnp.concatenate([norm, norm], axis=0)
        exchange(norm_slot)

    with scope("arrivep"):
        arrive(pick_slot)
    with scope("weights"):
        picked = tree(jnp.add, [comm[pick_slot, p] for p in range(vocab)])
        length_row = jnp.zeros((1, LANES), jnp.int32)
        places = []
        for n in range(seqs):
            rank = jnp.int32(0)
            for i in range(n):
                rank = rank + jnp.where(own[i] == own[n], 1, 0)
            places.append(own[n] * capacity + rank)
            length_row = jnp.where(lane_n == n, lens[n], length_row)
        live = lane_j < length_row
        safe_draft = jnp.where(live, picked[1:2], 1.0)
        accept = jnp.where(live, jnp.minimum(1.0, jnp.exp(picked[0:1] - peak_row) / total_row / safe_draft), 0.0)
        wide = jnp.broadcast_to(accept, (depth, LANES))
        before = tree(jnp.multiply, [
            jnp.where(lane_j >= k, pltpu.roll(wide, k, 1)[0:1], 1.0) for k in range(1, depth)
        ])
        weight = jnp.where(live, before * (1.0 - accept), 0.0)
        survive = before * accept
        inner = lax.broadcasted_iota(jnp.int32, (slots, TERMS * rows), 1)
        outer = lax.broadcasted_iota(jnp.int32, (slots, TERMS * rows), 0)
        picker = jnp.zeros((slots, TERMS * rows), jnp.float32)
        for n in range(seqs):
            picker = jnp.where((lax.rem(inner // depth, seqs) == n) & (outer == places[n]), 1.0, picker)
        picker = picker.astype(jnp.bfloat16)
    with scope("smallsend"):
        sent = zero
        for n in range(seqs):
            sent = jnp.where(lane == places[n], to_column(accept, n), sent)
            alive = jnp.where((lane_n == n) & (row_lane < rows), survive, 0.0)
            sent = jnp.where(lane == places[n] + half, jnp.sum(alive, axis=1, keepdims=True), sent)
        for g in range(groups):
            shift = (LANES - g * capacity) % LANES
            small[g] = pltpu.roll(sent, shift, 1) if shift else sent
        for to in g_peers:
            pltpu.make_async_remote_copy(
                src_ref=small.at[to], dst_ref=small_in.at[my_dp], send_sem=sm_ssem, recv_sem=sm_rsem,
                device_id=(to, my_v), device_id_type=MESH,
            ).start()
        small_in[my_dp] = small[my_dp]

    with scope("arrive2"):
        arrive(norm_slot)
    with scope("coef"):
        coef = weight / tree(jnp.add, [comm[norm_slot, p][0:1] for p in range(vocab)])
        coefs = [to_column(coef, n) for n in range(seqs)]
        lowers = [coefs[n] * (scales[n] * mixing) for n in range(seqs)]
        uppers = [coefs[n] * (scales[n] * (1.0 + mixing)) for n in range(seqs)]

    bounds = plan(tiles)
    chunks = len(bounds) - 1

    def pieces(c):
        whole = min(bounds[c + 1], full)
        found = [(bounds[c] + a, size) for a, size in slabs(whole - bounds[c], PIECE)]
        return found + ([(full, 1)] if bounds[c + 1] > full else [])

    def span(c):
        return pl.ds(bounds[c] * LANES, (bounds[c + 1] - bounds[c]) * LANES)

    square = groups == 4
    near, far, across = xor(my_dp, 1), xor(my_dp, 2), xor(my_dp, 3)

    def ship(c, to):
        pltpu.make_async_remote_copy(
            src_ref=send.at[to, :, span(c)], dst_ref=landed.at[my_dp, :, span(c)],
            send_sem=out_ssem, recv_sem=out_rsem.at[c],
            device_id=(to, my_v), device_id_type=MESH,
        ).start()

    for c in range(chunks):
        with scope(f"mix{c}"):
            for start, size in pieces(c):
                columns = pl.ds(start * LANES, size * LANES)
                values = []
                for n in range(seqs):
                    value = e[n, :, columns]
                    draft = tail_tile(d, n, 0.0) if start >= full else d[n, :, columns].astype(jnp.float32)
                    values.append(jnp.maximum(value * uppers[n] - draft * coefs[n], value * lowers[n]))
                value = jnp.concatenate(values, axis=0)
                terms = []
                for _ in range(TERMS):
                    terms.append(value.astype(jnp.bfloat16))
                    value = value - terms[-1].astype(jnp.float32)
                mixed = jnp.dot(picker, jnp.concatenate(terms, axis=0), preferred_element_type=jnp.float32)
                for g in range(groups):
                    send[g, :, columns] = mixed[g * capacity:(g + 1) * capacity].astype(jnp.bfloat16)
            if square:
                ship(c, far)

                @pl.when(across < near)
                def _():
                    ship(c, across)

                @pl.when(jnp.logical_not(across < near))
                def _():
                    ship(c, near)
            else:
                for to in g_peers:
                    ship(c, to)
            landed[my_dp, :, span(c)] = send[my_dp, :, span(c)]

    if square:
        @pl.when(across < near)
        def _():
            for c in range(chunks):
                ship(c, near)

        @pl.when(jnp.logical_not(across < near))
        def _():
            for c in range(chunks):
                ship(c, across)

    with scope("smallrecv"):
        others = pl.ds(0, groups - 1)
        pltpu.make_async_remote_copy(
            src_ref=small.at[others], dst_ref=small_in.at[others], send_sem=sm_ssem, recv_sem=sm_rsem,
            device_id=(g_peers[0], my_v), device_id_type=MESH,
        ).wait()
        final = zero
        for g in range(groups):
            mine = lax.rem(lane, half) // capacity == g
            final = jnp.where(mine, pltpu.roll(small_in[g], g * capacity, 1), final)
        accept_out[...] = final[:, :slots]
        expected_out[...] = final[0:1, half:half + slots]

    for c in range(chunks):
        with scope(f"recv{c}"):
            pltpu.make_async_remote_copy(
                src_ref=send.at[others, :, span(c)], dst_ref=landed.at[others, :, span(c)],
                send_sem=out_ssem, recv_sem=out_rsem.at[c],
                device_id=(g_peers[0], my_v), device_id_type=MESH,
            ).wait_recv()
        with scope(f"gather{c}"):
            for a, size in slabs(bounds[c + 1] - bounds[c], SLAB):
                start = (bounds[c] + a) * LANES
                columns = pl.ds(start, size * LANES)
                pieces = [landed[g, :, columns].astype(jnp.float32) for g in range(groups)]
                whole = jnp.concatenate(pieces, axis=0).astype(jnp.bfloat16)
                kept = min(size * LANES, width - start)
                block[:, pl.ds(start, kept)] = whole[:, :kept]
    with scope("sendwait"):
        pltpu.make_async_remote_copy(
            src_ref=send.at[others], dst_ref=landed.at[others], send_sem=out_ssem, recv_sem=out_rsem.at[0],
            device_id=(g_peers[0], my_v), device_id_type=MESH,
        ).wait_send()
        others = comm.at[:, pl.ds(0, vocab - 1)]
        pltpu.make_async_remote_copy(
            src_ref=others, dst_ref=others, send_sem=comm_ssem, recv_sem=comm_rsem.at[0],
            device_id=(my_dp, v_peers[0]), device_id_type=MESH,
        ).wait_send()


def finish(block, accept, expected, out, accept_out, expected_out, sem):
    step = -(-block.shape[1] // (PARTS * LANES)) * LANES
    spans = [pl.ds(a, min(step, block.shape[1] - a)) for a in range(0, block.shape[1], step)]
    pairs = [(block.at[:, c], out.at[:, c]) for c in spans] + [(accept, accept_out), (expected, expected_out)]
    copies = [pltpu.make_async_copy(a, b, sem.at[i]) for i, (a, b) in enumerate(pairs)]
    for copy in copies:
        copy.start()
    for copy in copies:
        copy.wait()


def body(logits, draft_probs, draft_tokens, draft_lengths, owner_group):
    groups = lax.axis_size("dp")
    vocab = lax.axis_size("vocab")
    seqs, depth, width = logits.shape
    capacity = max(2, 2 * seqs // groups)
    tiles = -(-width // LANES)
    padded = tiles * LANES
    chunks = len(plan(tiles)) - 1
    hbm = pl.BlockSpec(memory_space=pltpu.HBM)
    vmem = pl.BlockSpec(memory_space=pltpu.VMEM)
    dma = pltpu.SemaphoreType.DMA
    slots = groups * capacity
    shapes = (
        jax.ShapeDtypeStruct((slots, width), jnp.bfloat16),
        jax.ShapeDtypeStruct((depth, slots), jnp.float32),
        jax.ShapeDtypeStruct((1, slots), jnp.float32),
    )
    outs = pl.pallas_call(
        functools.partial(kernel, (groups, vocab, capacity)),
        out_shape=shapes,
        in_specs=[hbm] * 5,
        out_specs=(vmem, vmem, vmem),
        scratch_shapes=[
            pltpu.SMEM((seqs, depth), jnp.int32),
            pltpu.SMEM((seqs,), jnp.int32),
            pltpu.SMEM((seqs,), jnp.int32),
            pltpu.VMEM((seqs, depth, width), jnp.bfloat16),
            pltpu.VMEM((seqs, depth, width), jnp.bfloat16),
            pltpu.VMEM((seqs, depth, padded), jnp.float32),
            pltpu.VMEM((groups, capacity, padded), jnp.bfloat16),
            pltpu.VMEM((groups, capacity, padded), jnp.bfloat16),
            pltpu.VMEM((BATCHES + 2, vocab, 2, LANES), jnp.float32),
            pltpu.VMEM((groups, depth, LANES), jnp.float32),
            pltpu.VMEM((groups, depth, LANES), jnp.float32),
            dma((3,)),
            dma((len(slabs(seqs, PAIR)),)),
            dma(()),
            dma(()),
            dma((BATCHES + 2,)),
            dma(()),
            dma((chunks,)),
            dma(()),
            dma(()),
        ],
        compiler_params=pltpu.CompilerParams(
            collective_id=0, has_side_effects=True, vmem_limit_bytes=54500 * 1024
        ),
    )(*[pltpu.with_memory_space_constraint(a, pltpu.HBM) for a in (draft_tokens, draft_lengths, owner_group)], logits, draft_probs)
    out, accept, expected = pl.pallas_call(
        finish,
        out_shape=shapes,
        in_specs=[vmem] * 3,
        out_specs=(hbm, hbm, hbm),
        scratch_shapes=[dma((PARTS + 2,))],
        compiler_params=pltpu.CompilerParams(vmem_limit_bytes=1024 * 1024),
    )(*outs)
    return (out, accept.T, expected.reshape(slots))


def solution(mesh):
    placed = (P("dp", None, "vocab"), P("dp", None, "vocab"), P("dp", None), P("dp"), P("dp"))
    return jax.shard_map(
        body,
        mesh=mesh,
        in_specs=placed,
        out_specs=(P("dp", "vocab"), P("dp", None), P("dp")),
        check_vma=False,
    )
```

```python
import functools

import jax
import jax.numpy as jnp
from jax import lax
from jax.experimental import pallas as pl
from jax.experimental.pallas import tpu as pltpu
from jax.sharding import PartitionSpec as P

mixing = 0.1
LANES = 128
SLAB = 8
PIECE = 2
BATCHES = 1
TERMS = 3
PARTS = 1
PAIR = 2
FIRST = 2
GROWTH = 3
MOST = 24
LOW = -1e30
MESH = pl.DeviceIdType.MESH
scope = jax.named_scope


def slabs(full, size):
    return [(a, min(size, full - a)) for a in range(0, full, size)]


def plan(tiles):
    bounds, size = [0], FIRST
    while bounds[-1] < tiles:
        bounds.append(min(tiles, bounds[-1] + size))
        size = min(size * GROWTH, MOST)
    return bounds


def landings(chunks):
    cuts = sorted({0, max(0, chunks - 4), max(0, chunks - 2), max(0, chunks - 1), chunks})
    return list(zip(cuts[:-1], cuts[1:]))


def xor(value, mask):
    bit = 1
    while bit <= mask:
        if mask & bit:
            value = value + bit - 2 * bit * lax.rem(value // bit, 2)
        bit *= 2
    return value


def partners(me, count):
    if count & (count - 1):
        return [lax.rem(me + k, count) for k in range(1, count)]
    return [xor(me, k) for k in range(count - 1, 0, -1)]


def by_distance(me, count):
    picks = [jnp.where(2 * me < count, count - 2 - i, i) for i in range(count - 1)]
    return [p + jnp.where(p >= me, 1, 0) for p in picks]


def tree(op, values):
    values = list(values)
    while len(values) > 1:
        values = [op(*values[i:i + 2]) if i + 1 < len(values) else values[i] for i in range(0, len(values), 2)]
    return values[0]


def kernel(
    dims,
    tok_hbm, lens_hbm, own_hbm, x_hbm, d_hbm,
    block, accept_out, expected_out,
    tok, lens, own, x, d, e, send, landed, comm, small, small_in,
    scalar_sem, x_sem, d_sem, comm_ssem, comm_rsem, out_ssem, out_rsem, sm_ssem, sm_rsem,
):
    groups, vocab, capacity = dims
    seqs, depth, width = x_hbm.shape
    full = width // LANES
    tail = width - full * LANES
    tiles = e.shape[2] // LANES
    rows = seqs * depth
    slots = groups * capacity
    half = LANES // 2
    pick_slot, norm_slot = BATCHES, BATCHES + 1
    my_dp = lax.axis_index("dp")
    my_v = lax.axis_index("vocab")

    barrier = pltpu.get_barrier_semaphore()
    v_peers = by_distance(my_v, vocab)
    g_peers = partners(my_dp, groups)
    for p in v_peers:
        pl.semaphore_signal(barrier, inc=1, device_id=(my_dp, p), device_id_type=MESH)
    for p in g_peers:
        pl.semaphore_signal(barrier, inc=1, device_id=(p, my_v), device_id_type=MESH)

    pairs = slabs(seqs, PAIR)
    x_loads, d_loads = [], []
    for i, (n, size) in enumerate(pairs):
        part = pl.ds(n, size)
        x_loads.append(pltpu.make_async_copy(x_hbm.at[part], x.at[part], x_sem.at[i]))
        d_loads.append(pltpu.make_async_copy(d_hbm.at[part], d.at[part], d_sem))
        x_loads[-1].start()
    scalars = []
    for i, (source, target) in enumerate(((tok_hbm, tok), (lens_hbm, lens), (own_hbm, own))):
        scalars.append(pltpu.make_async_copy(source, target, scalar_sem.at[i]))
        scalars[-1].start()

    sub = lax.broadcasted_iota(jnp.int32, (depth, LANES), 0)
    lane = lax.broadcasted_iota(jnp.int32, (depth, LANES), 1)
    row_lane = lax.broadcasted_iota(jnp.int32, (1, LANES), 1)
    lane_j = lax.rem(row_lane, depth)
    lane_n = lax.rem(row_lane // depth, seqs)
    zero = jnp.zeros((depth, LANES), jnp.float32)
    spots = [(lax.rem(lane, depth) == sub) & (lax.rem(lane // depth, seqs) == n) for n in range(seqs)]

    def tail_tile(ref, n, fill):
        part = ref[n, :, pl.ds(full * LANES, tail)].astype(jnp.float32)
        return jnp.concatenate([part, jnp.full((depth, LANES - tail), fill, jnp.float32)], axis=1)

    def to_row(columns):
        spread = zero
        for n, column in columns.items():
            spread = jnp.where(spots[n], column, spread)
        return jnp.sum(spread, axis=0, keepdims=True)

    def to_column(row, n):
        placed = jnp.where(spots[n] & (lane < rows), row, 0.0)
        return jnp.sum(placed, axis=1, keepdims=True)

    def exchange(slot):
        for to in v_peers:
            pltpu.make_async_remote_copy(
                src_ref=comm.at[slot, my_v], dst_ref=comm.at[slot, my_v],
                send_sem=comm_ssem, recv_sem=comm_rsem.at[slot],
                device_id=(my_dp, to), device_id_type=MESH,
            ).start()

    def arrive(slot):
        others = comm.at[slot, pl.ds(0, vocab - 1)]
        pltpu.make_async_remote_copy(
            src_ref=others, dst_ref=others, send_sem=comm_ssem, recv_sem=comm_rsem.at[slot],
            device_id=(my_dp, v_peers[0]), device_id_type=MESH,
        ).wait_recv()

    def peak(n):
        wide = 2 * LANES
        running = [x[n, :, pl.ds(k * wide, wide)] for k in range(min(4, full // 2))]
        for k in range(4, full // 2):
            running[k % 4] = jnp.maximum(running[k % 4], x[n, :, pl.ds(k * wide, wide)])
        top = tree(jnp.maximum, running).astype(jnp.float32)
        top = jnp.maximum(top[:, :LANES], top[:, LANES:])
        if full % 2:
            top = jnp.maximum(top, x[n, :, pl.ds((full - 1) * LANES, LANES)].astype(jnp.float32))
        if tail:
            top = jnp.maximum(top, tail_tile(x, n, LOW))
        return jnp.max(top, axis=1, keepdims=True)

    def expo(n, top):
        parts = [zero] * 4
        for a, size in slabs(full, SLAB):
            raw = x[n, :, pl.ds(a * LANES, size * LANES)].astype(jnp.float32)
            value = jnp.exp(raw - top)
            e[n, :, pl.ds(a * LANES, size * LANES)] = value
            for k in range(size):
                parts[k % 4] = parts[k % 4] + value[:, k * LANES:(k + 1) * LANES]
        if tail:
            value = jnp.exp(tail_tile(x, n, LOW) - top)
            e[n, :, pl.ds(full * LANES, LANES)] = value
            parts[0] = parts[0] + value
        return jnp.sum((parts[0] + parts[1]) + (parts[2] + parts[3]), axis=1, keepdims=True)

    tops, sums = {}, {}

    def take(i):
        n, size = pairs[i]
        with scope(f"load{i}"):
            x_loads[i].wait()
            if i == 0:
                for load in d_loads:
                    load.start()
        with scope(f"peak{i}"):
            for m in range(n, n + size):
                tops[m] = peak(m)

    take(0)
    for i, (n, size) in enumerate(pairs):
        if i + 1 < len(pairs):
            take(i + 1)
        with scope(f"expo{i}"):
            for m in range(n, n + size):
                sums[m] = expo(m, tops[m])
    with scope("send1"):
        comm[0, my_v] = jnp.concatenate([to_row(tops), to_row(sums)], axis=0)
    with scope("barrier"):
        pl.semaphore_wait(barrier, vocab - 1 + groups - 1)
        exchange(0)

    with scope("pick"):
        column0 = my_v * width
        chosen, drafted, masses = {}, {}, {}
        for copy in scalars:
            copy.wait()
        pltpu.make_async_copy(d_hbm, d, d_sem).wait()
        for n in range(seqs):
            spot = jnp.zeros((depth, LANES), jnp.int32)
            for j in range(depth):
                spot = jnp.where(sub == j, tok[n, j], spot)
            spot = spot - column0 - lane
            hit_x, hit_d, mass = zero, zero, [zero] * 4
            if tail:
                hit = (spot == full * LANES) & (lane < tail)
                hit_x = jnp.where(hit, tail_tile(x, n, 0.0), hit_x)
                hit_d = jnp.where(hit, tail_tile(d, n, 0.0), hit_d)
                mass[0] = tail_tile(d, n, 0.0)
            for a, size in slabs(full, SLAB):
                columns = pl.ds(a * LANES, size * LANES)
                raw_x, raw_d = x[n, :, columns].astype(jnp.float32), d[n, :, columns].astype(jnp.float32)
                for k in range(size):
                    hit = spot == (a + k) * LANES
                    hit_x = jnp.where(hit, raw_x[:, k * LANES:(k + 1) * LANES], hit_x)
                    hit_d = jnp.where(hit, raw_d[:, k * LANES:(k + 1) * LANES], hit_d)
                    mass[k % 4] = mass[k % 4] + raw_d[:, k * LANES:(k + 1) * LANES]
            chosen[n] = jnp.sum(hit_x, axis=1, keepdims=True)
            drafted[n] = jnp.sum(hit_d, axis=1, keepdims=True)
            masses[n] = (mass[0] + mass[1]) + (mass[2] + mass[3])
        comm[pick_slot, my_v] = jnp.concatenate([to_row(chosen), to_row(drafted)], axis=0)
        exchange(pick_slot)

    with scope("arrive1"):
        arrive(0)
    with scope("merge"):
        parts = [comm[0, p] for p in range(vocab)]
        peak_row = tree(jnp.maximum, [part[0:1] for part in parts])
        total_row = tree(jnp.add, [part[1:2] * jnp.exp(part[0:1] - peak_row) for part in parts])
        mine = comm[0, my_v]
        scale = jnp.exp(mine[0:1] - peak_row) / total_row
        scales = [to_column(scale, n) for n in range(seqs)]
    excess = {}
    for n in range(seqs):
        with scope(f"gap{n}"):
            parts = [zero] * 4
            for a, size in slabs(full, SLAB):
                columns = pl.ds(a * LANES, size * LANES)
                upper = jnp.maximum(e[n, :, columns] * scales[n], d[n, :, columns].astype(jnp.float32))
                for k in range(size):
                    parts[k % 4] = parts[k % 4] + upper[:, k * LANES:(k + 1) * LANES]
            if tail:
                parts[0] = parts[0] + jnp.maximum(e[n, :, pl.ds(full * LANES, LANES)] * scales[n], tail_tile(d, n, 0.0))
            total = (parts[0] + parts[1]) + (parts[2] + parts[3])
            excess[n] = jnp.sum(total - masses[n], axis=1, keepdims=True)
    with scope("send2"):
        norm = to_row(excess) + mixing * scale * mine[1:2]
        comm[norm_slot, my_v] = jnp.concatenate([norm, norm], axis=0)
        exchange(norm_slot)

    with scope("arrivep"):
        arrive(pick_slot)
    with scope("weights"):
        picked = tree(jnp.add, [comm[pick_slot, p] for p in range(vocab)])
        length_row = jnp.zeros((1, LANES), jnp.int32)
        places = []
        for n in range(seqs):
            rank = jnp.int32(0)
            for i in range(n):
                rank = rank + jnp.where(own[i] == own[n], 1, 0)
            places.append(own[n] * capacity + rank)
            length_row = jnp.where(lane_n == n, lens[n], length_row)
        live = lane_j < length_row
        safe_draft = jnp.where(live, picked[1:2], 1.0)
        accept = jnp.where(live, jnp.minimum(1.0, jnp.exp(picked[0:1] - peak_row) / total_row / safe_draft), 0.0)
        wide = jnp.broadcast_to(accept, (depth, LANES))
        before = tree(jnp.multiply, [
            jnp.where(lane_j >= k, pltpu.roll(wide, k, 1)[0:1], 1.0) for k in range(1, depth)
        ])
        weight = jnp.where(live, before * (1.0 - accept), 0.0)
        survive = before * accept
        inner = lax.broadcasted_iota(jnp.int32, (slots, TERMS * rows), 1)
        outer = lax.broadcasted_iota(jnp.int32, (slots, TERMS * rows), 0)
        picker = jnp.zeros((slots, TERMS * rows), jnp.float32)
        for n in range(seqs):
            picker = jnp.where((lax.rem(inner // depth, seqs) == n) & (outer == places[n]), 1.0, picker)
        picker = picker.astype(jnp.bfloat16)
    with scope("smallsend"):
        sent = zero
        for n in range(seqs):
            sent = jnp.where(lane == places[n], to_column(accept, n), sent)
            alive = jnp.where((lane_n == n) & (row_lane < rows), survive, 0.0)
            sent = jnp.where(lane == places[n] + half, jnp.sum(alive, axis=1, keepdims=True), sent)
        for g in range(groups):
            shift = (LANES - g * capacity) % LANES
            small[g] = pltpu.roll(sent, shift, 1) if shift else sent
        for to in g_peers:
            pltpu.make_async_remote_copy(
                src_ref=small.at[to], dst_ref=small_in.at[my_dp], send_sem=sm_ssem, recv_sem=sm_rsem,
                device_id=(to, my_v), device_id_type=MESH,
            ).start()
        small_in[my_dp] = small[my_dp]

    with scope("arrive2"):
        arrive(norm_slot)
    with scope("coef"):
        coef = weight / tree(jnp.add, [comm[norm_slot, p][0:1] for p in range(vocab)])
        coefs = [to_column(coef, n) for n in range(seqs)]
        lowers = [coefs[n] * (scales[n] * mixing) for n in range(seqs)]
        uppers = [coefs[n] * (scales[n] * (1.0 + mixing)) for n in range(seqs)]

    bounds = plan(tiles)
    chunks = len(bounds) - 1

    def pieces(c):
        whole = min(bounds[c + 1], full)
        found = [(bounds[c] + a, size) for a, size in slabs(whole - bounds[c], PIECE)]
        return found + ([(full, 1)] if bounds[c + 1] > full else [])

    groups_of = landings(chunks)

    def landing(c):
        return [first <= c < last for first, last in groups_of].index(True)

    def span(c, last=None):
        last = c + 1 if last is None else last
        return pl.ds(bounds[c] * LANES, (bounds[last] - bounds[c]) * LANES)

    square = groups == 4
    near, far, across = xor(my_dp, 1), xor(my_dp, 2), xor(my_dp, 3)

    def ship(c, to):
        pltpu.make_async_remote_copy(
            src_ref=send.at[to, :, span(c)], dst_ref=landed.at[my_dp, :, span(c)],
            send_sem=out_ssem, recv_sem=out_rsem.at[landing(c)],
            device_id=(to, my_v), device_id_type=MESH,
        ).start()

    for c in range(chunks):
        with scope(f"mix{c}"):
            for start, size in pieces(c):
                columns = pl.ds(start * LANES, size * LANES)
                values = []
                for n in range(seqs):
                    value = e[n, :, columns]
                    draft = tail_tile(d, n, 0.0) if start >= full else d[n, :, columns].astype(jnp.float32)
                    values.append(jnp.maximum(value * uppers[n] - draft * coefs[n], value * lowers[n]))
                value = jnp.concatenate(values, axis=0)
                terms = []
                for _ in range(TERMS):
                    terms.append(value.astype(jnp.bfloat16))
                    value = value - terms[-1].astype(jnp.float32)
                mixed = jnp.dot(picker, jnp.concatenate(terms, axis=0), preferred_element_type=jnp.float32)
                for g in range(groups):
                    send[g, :, columns] = mixed[g * capacity:(g + 1) * capacity].astype(jnp.bfloat16)
            if square:
                ship(c, far)

                @pl.when(across < near)
                def _():
                    ship(c, across)

                @pl.when(jnp.logical_not(across < near))
                def _():
                    ship(c, near)
            else:
                for to in g_peers:
                    ship(c, to)
            landed[my_dp, :, span(c)] = send[my_dp, :, span(c)]

    if square:
        @pl.when(across < near)
        def _():
            for c in range(chunks):
                ship(c, near)

        @pl.when(jnp.logical_not(across < near))
        def _():
            for c in range(chunks):
                ship(c, across)

    with scope("smallrecv"):
        others = pl.ds(0, groups - 1)
        pltpu.make_async_remote_copy(
            src_ref=small.at[others], dst_ref=small_in.at[others], send_sem=sm_ssem, recv_sem=sm_rsem,
            device_id=(g_peers[0], my_v), device_id_type=MESH,
        ).wait()
        final = zero
        for g in range(groups):
            mine = lax.rem(lane, half) // capacity == g
            final = jnp.where(mine, pltpu.roll(small_in[g], g * capacity, 1), final)
        accept_out[...] = final[:, :slots]
        expected_out[...] = final[0:1, half:half + slots]

    for i, (c, last) in enumerate(groups_of):
        with scope(f"recv{c}"):
            pltpu.make_async_remote_copy(
                src_ref=send.at[others, :, span(c, last)], dst_ref=landed.at[others, :, span(c, last)],
                send_sem=out_ssem, recv_sem=out_rsem.at[i],
                device_id=(g_peers[0], my_v), device_id_type=MESH,
            ).wait_recv()
        with scope(f"gather{c}"):
            for a, size in slabs(bounds[last] - bounds[c], SLAB):
                start = (bounds[c] + a) * LANES
                columns = pl.ds(start, size * LANES)
                pieces = [landed[g, :, columns].astype(jnp.float32) for g in range(groups)]
                whole = jnp.concatenate(pieces, axis=0).astype(jnp.bfloat16)
                kept = min(size * LANES, width - start)
                block[:, pl.ds(start, kept)] = whole[:, :kept]
    with scope("sendwait"):
        pltpu.make_async_remote_copy(
            src_ref=send.at[others], dst_ref=landed.at[others], send_sem=out_ssem, recv_sem=out_rsem.at[0],
            device_id=(g_peers[0], my_v), device_id_type=MESH,
        ).wait_send()
        others = comm.at[:, pl.ds(0, vocab - 1)]
        pltpu.make_async_remote_copy(
            src_ref=others, dst_ref=others, send_sem=comm_ssem, recv_sem=comm_rsem.at[0],
            device_id=(my_dp, v_peers[0]), device_id_type=MESH,
        ).wait_send()


def finish(block, accept, expected, out, accept_out, expected_out, sem):
    step = -(-block.shape[1] // (PARTS * LANES)) * LANES
    spans = [pl.ds(a, min(step, block.shape[1] - a)) for a in range(0, block.shape[1], step)]
    pairs = [(block.at[:, c], out.at[:, c]) for c in spans] + [(accept, accept_out), (expected, expected_out)]
    copies = [pltpu.make_async_copy(a, b, sem.at[i]) for i, (a, b) in enumerate(pairs)]
    for copy in copies:
        copy.start()
    for copy in copies:
        copy.wait()


def body(logits, draft_probs, draft_tokens, draft_lengths, owner_group):
    groups = lax.axis_size("dp")
    vocab = lax.axis_size("vocab")
    seqs, depth, width = logits.shape
    capacity = max(2, 2 * seqs // groups)
    tiles = -(-width // LANES)
    padded = tiles * LANES
    chunks = len(plan(tiles)) - 1
    hbm = pl.BlockSpec(memory_space=pltpu.HBM)
    vmem = pl.BlockSpec(memory_space=pltpu.VMEM)
    dma = pltpu.SemaphoreType.DMA
    slots = groups * capacity
    shapes = (
        jax.ShapeDtypeStruct((slots, width), jnp.bfloat16),
        jax.ShapeDtypeStruct((depth, slots), jnp.float32),
        jax.ShapeDtypeStruct((1, slots), jnp.float32),
    )
    outs = pl.pallas_call(
        functools.partial(kernel, (groups, vocab, capacity)),
        out_shape=shapes,
        in_specs=[hbm] * 5,
        out_specs=(vmem, vmem, vmem),
        scratch_shapes=[
            pltpu.SMEM((seqs, depth), jnp.int32),
            pltpu.SMEM((seqs,), jnp.int32),
            pltpu.SMEM((seqs,), jnp.int32),
            pltpu.VMEM((seqs, depth, width), jnp.bfloat16),
            pltpu.VMEM((seqs, depth, width), jnp.bfloat16),
            pltpu.VMEM((seqs, depth, padded), jnp.float32),
            pltpu.VMEM((groups, capacity, padded), jnp.bfloat16),
            pltpu.VMEM((groups, capacity, padded), jnp.bfloat16),
            pltpu.VMEM((BATCHES + 2, vocab, 2, LANES), jnp.float32),
            pltpu.VMEM((groups, depth, LANES), jnp.float32),
            pltpu.VMEM((groups, depth, LANES), jnp.float32),
            dma((3,)),
            dma((len(slabs(seqs, PAIR)),)),
            dma(()),
            dma(()),
            dma((BATCHES + 2,)),
            dma(()),
            dma((len(landings(chunks)),)),
            dma(()),
            dma(()),
        ],
        compiler_params=pltpu.CompilerParams(
            collective_id=0, has_side_effects=True, vmem_limit_bytes=54500 * 1024
        ),
    )(*[pltpu.with_memory_space_constraint(a, pltpu.HBM) for a in (draft_tokens, draft_lengths, owner_group)], logits, draft_probs)
    out, accept, expected = pl.pallas_call(
        finish,
        out_shape=shapes,
        in_specs=[vmem] * 3,
        out_specs=(hbm, hbm, hbm),
        scratch_shapes=[dma((PARTS + 2,))],
        compiler_params=pltpu.CompilerParams(vmem_limit_bytes=1024 * 1024),
    )(*outs)
    return (out, accept.T, expected.reshape(slots))


def solution(mesh):
    placed = (P("dp", None, "vocab"), P("dp", None, "vocab"), P("dp", None), P("dp"), P("dp"))
    return jax.shard_map(
        body,
        mesh=mesh,
        in_specs=placed,
        out_specs=(P("dp", "vocab"), P("dp", None), P("dp")),
        check_vma=False,
    )
```
